32 devices in a mesh: groups: 2 (over x), patch: 16 (over z, y, core).
Axes of the slice: x: 2, y: 2, z: 4, core: 2. Of those that a mesh axis runs over, the one named last changes fastest.
Arguments:
- tokens: bfloat16 [16384, 1152], P(('groups', 'patch')), parts along dimension 0, may hold values from -6 to 6
- stale_kv: bfloat16 [16384, 1152], P(('groups', 'patch')), parts along dimension 0, may hold values from -40 to 40, as said below
- mod_table: float32 [6, 1152], replicated, may hold values from -2 to 3
- mod_mix: float32 [6, 1152], replicated, may hold values from -3 to 3
- timestep: int32 [2], P('groups'), parts along dimension 0, may hold values from 0 to 999
- frame_order: int32 [8], P('groups'), parts along dimension 0, may hold values from 0 to 3, each once
- spatial_qkv: bfloat16 [3, 1152, 576], replicated, may hold values from -0.1875 to 0.1875
- spatial_out: bfloat16 [576, 1152], replicated, may hold values from -0.25 to 0.25
- temporal_qkv: bfloat16 [3, 1152, 576], replicated, may hold values from -0.1875 to 0.1875
- temporal_out: bfloat16 [576, 1152], replicated, may hold values from -0.25 to 0.25
Outputs:
- block_out: float32 [16384, 1152], P(('groups', 'patch')), parts along dimension 0
The draws below stay inside these ranges and needn't reach their ends.
There are 2 independent parts, one for each index of `groups`. The reference program is written for one: setup_inputs(seed, part) draws one part's arguments, and reference() takes and returns one part's arrays. A program takes and returns all parts, laid end to end along the dimension named above; an argument that names none is the same for every part. Nothing has to cross between parts.
Inputs may be any that keep to these rules, and one draw needn't show every extreme that they name: `frame_order`: a permutation of the 4 time positions. `stale_kv`: previous step's keys and values.
All inputs are finite; a program needn't handle non-finite values.
Results may differ from the reference program's by a relative error of at most 0.013.
The reference program's roundings to bfloat16 on the way count: a program that leaves them out, or rounds other values in their place, can miss the bound.
Values may be sent and summed in bfloat16 or wider, within the bound.
A program may use at most 128 MiB of HBM per device.

```python
import math
import jax
import jax.numpy as jnp
from jax import lax

D = 1152
HEADS = 16
HEADS_WIN = 8
WIN = 576
PATCH_TOK = 512
FRAMES = 4
FRAME_TOK = 2048
TOKENS = 8192


def draw_stale_kv(key, part):
    width_win = HEADS_WIN * (D // HEADS)
    base = jnp.clip(jax.random.normal(jax.random.fold_in(key, 11), (TOKENS, 2 * width_win), jnp.float32), -5.0, 5.0)
    return base.astype(jnp.bfloat16)


def draw_mod_table(key, part):
    table = jnp.clip(0.5 * jax.random.normal(jax.random.fold_in(key, 21), (6, D), jnp.float32), -2.0, 2.0)
    return table


def levels(rng, shape, split, smallest, largest):
    loudness, own = 1.0, jax.random.fold_in(rng, 6)
    for axis_at, blocks in split:
        heights = jnp.exp(jax.random.uniform(jax.random.fold_in(own, axis_at), (blocks,), jnp.float32, smallest / len(split), largest / len(split)))
        loudness = loudness * jnp.repeat(heights, shape[axis_at] // blocks).reshape([-1 if axis == axis_at else 1 for axis in range(len(shape))])
    return loudness


def scatter_about(own_key, shape, width, limit, shards=(), kind=jnp.bfloat16):
    entries = jax.random.normal(own_key, shape, jnp.float32) * width
    if len(shards) > 0:
        entries = levels(own_key, shape, shards, -0.22, 0.18) * entries
    return jnp.clip(entries, min=-limit, max=limit).astype(kind)


def setup_inputs(seed: int = 0, part: int = 0) -> dict:
    key_list = jax.random.split(jax.random.key(seed), 11)
    part_keys = jax.random.split(jax.random.fold_in(key_list[10], part), 11)
    tokens = scatter_about(part_keys[0], (TOKENS, D), 1.0, 6.0, ((0, 16),))
    stale_kv = draw_stale_kv(jax.random.fold_in(jax.random.fold_in(key_list[10], part), 71), part)
    mod_table = draw_mod_table(jax.random.fold_in(key_list[10], 71), part)
    mod_mix = scatter_about(key_list[3], (6, D), 0.5, 3.0, (), jnp.float32)
    timestep = jax.random.randint(part_keys[4], (1,), 0, 1000).astype(jnp.int32)
    frame_order = jax.random.permutation(part_keys[5], FRAMES).astype(jnp.int32)
    spatial_qkv = scatter_about(key_list[6], (3, D, WIN), D ** -0.5, 0.1875)
    spatial_out = scatter_about(key_list[7], (WIN, D), WIN ** -0.5, 0.25)
    temporal_qkv = scatter_about(key_list[8], (3, D, WIN), D ** -0.5, 0.1875)
    temporal_out = scatter_about(key_list[9], (WIN, D), WIN ** -0.5, 0.25)
    return {"tokens": tokens, "stale_kv": stale_kv, "mod_table": mod_table, "mod_mix": mod_mix, "timestep": timestep, "frame_order": frame_order, "spatial_qkv": spatial_qkv, "spatial_out": spatial_out, "temporal_qkv": temporal_qkv, "temporal_out": temporal_out}


epsilon = 1e-06

def normalize(activations):
    row_mean = lax.optimization_barrier(jnp.mean(activations, axis=-1, keepdims=True))
    centered = activations - row_mean
    variance = lax.optimization_barrier(jnp.mean(centered * centered, axis=-1, keepdims=True))
    return centered * lax.rsqrt(variance + epsilon)

def sinusoid(position, feature_width):
    half_width = feature_width // 2
    frequencies = jnp.exp(-math.log(10000.0) * jnp.arange(half_width, dtype=jnp.float32) / half_width)
    angles = jnp.asarray(position).astype(jnp.float32)[..., None] * frequencies
    return jnp.concatenate([jnp.sin(angles), jnp.cos(angles)], axis=-1)

def softmax_rows(scores):
    row_top = lax.optimization_barrier(jnp.max(scores, axis=-1, keepdims=True))
    exp_scores = jnp.exp(scores - row_top)
    return (exp_scores / lax.optimization_barrier(jnp.sum(exp_scores, axis=-1, keepdims=True))).astype(jnp.bfloat16)

def project(inputs, weight):
    return jnp.dot(inputs, weight, preferred_element_type=jnp.float32)

def spatial_attend(queries, key_rows, value_rows):
    head_dim = D // HEADS
    query_heads = queries.reshape(-1, HEADS_WIN, head_dim).astype(jnp.float32)
    key_heads = key_rows.reshape(-1, HEADS_WIN, head_dim).astype(jnp.float32)
    value_heads = value_rows.reshape(-1, HEADS_WIN, head_dim).astype(jnp.float32)
    scores = jnp.einsum('qhe,khe->hqk', query_heads, key_heads) * head_dim ** (-0.5)
    weights = softmax_rows(scores)
    mixed_out = jnp.einsum('hqk,khe->qhe', weights.astype(jnp.float32), value_heads)
    return mixed_out.reshape(-1, HEADS_WIN * head_dim).astype(jnp.bfloat16)

def temporal_attend(queries, key_rows, value_rows):
    head_dim = D // HEADS
    frame_count = queries.shape[0]
    pixel_count = queries.shape[1]
    shape_heads = (frame_count, pixel_count, HEADS_WIN, head_dim)
    query_heads = queries.reshape(shape_heads).astype(jnp.float32)
    key_heads = key_rows.reshape(shape_heads).astype(jnp.float32)
    value_heads = value_rows.reshape(shape_heads).astype(jnp.float32)
    scores = jnp.einsum('fmhe,gmhe->mhfg', query_heads, key_heads) * head_dim ** (-0.5)
    weights = softmax_rows(scores)
    mixed_out = jnp.einsum('mhfg,gmhe->fmhe', weights.astype(jnp.float32), value_heads)
    return mixed_out.reshape(frame_count, pixel_count, HEADS_WIN * head_dim).astype(jnp.bfloat16)

def reference(tokens, stale_kv, mod_table, mod_mix, timestep, frame_order, spatial_qkv, spatial_out, temporal_qkv, temporal_out):
    width_win = HEADS_WIN * (D // HEADS)
    modulation = mod_table + mod_mix * sinusoid(timestep[0], D)[None, :]
    tokens_wide = tokens.astype(jnp.float32)
    spatial_in = (normalize(tokens_wide) * (1.0 + modulation[1]) + modulation[0]).astype(jnp.bfloat16)
    quartered = (FRAMES, 4, PATCH_TOK, width_win)
    fresh_q = project(spatial_in, spatial_qkv[0]).astype(jnp.bfloat16).reshape(quartered)
    fresh_k = project(spatial_in, spatial_qkv[1]).astype(jnp.bfloat16).reshape(quartered)
    fresh_v = project(spatial_in, spatial_qkv[2]).astype(jnp.bfloat16).reshape(quartered)
    stale_k = stale_kv[:, :width_win].reshape(quartered)
    stale_v = stale_kv[:, width_win:].reshape(quartered)

    def one_frame(inputs):
        frame_q, frame_k, frame_v, old_k, old_v = inputs
        results = []
        for quarter in range(4):
            key_rows = jnp.concatenate([frame_k[source] if source == quarter else old_k[source] for source in range(4)], axis=0)
            value_rows = jnp.concatenate([frame_v[source] if source == quarter else old_v[source] for source in range(4)], axis=0)
            results.append(spatial_attend(frame_q[quarter], key_rows, value_rows))
        return jnp.stack(results)
    spatial_mixed = lax.map(one_frame, (fresh_q, fresh_k, fresh_v, stale_k, stale_v)).reshape(TOKENS, width_win)
    after_spatial = tokens_wide + modulation[2] * project(spatial_mixed, spatial_out)
    positions = sinusoid(frame_order, D)
    temporal_in = normalize(after_spatial).reshape(FRAMES, FRAME_TOK, D) * (1.0 + modulation[4]) + modulation[3] + positions[:, None, :]
    temporal_in = temporal_in.astype(jnp.bfloat16).reshape(TOKENS, D)
    framed = (FRAMES, FRAME_TOK, width_win)
    temporal_q = project(temporal_in, temporal_qkv[0]).astype(jnp.bfloat16).reshape(framed)
    temporal_k = project(temporal_in, temporal_qkv[1]).astype(jnp.bfloat16).reshape(framed)
    temporal_v = project(temporal_in, temporal_qkv[2]).astype(jnp.bfloat16).reshape(framed)
    temporal_mixed = temporal_attend(temporal_q, temporal_k, temporal_v).reshape(TOKENS, width_win)
    return after_spatial + modulation[5] * project(temporal_mixed, temporal_out)
```

```python
import functools
import math

import jax
import jax.numpy as jnp
from jax import lax
from jax.experimental import pallas as pl
from jax.experimental.pallas import tpu as pltpu
from jax.sharding import PartitionSpec as P

HEADS = 16
LANES = 128

epsilon = 1e-06


def swap_bit(value, axis, distance):
    mask = 2**distance
    pairs = [(source, source ^ mask) for source in range(lax.axis_size(axis))]
    return lax.ppermute(value, axis, pairs)


def normalize(activations):
    row_mean = jnp.mean(activations, axis=-1, keepdims=True)
    centered = activations - row_mean
    variance = jnp.mean(centered * centered, axis=-1, keepdims=True)
    return centered * lax.rsqrt(variance + epsilon)


def sinusoid(position, feature_width):
    half_width = feature_width // 2
    frequencies = jnp.exp(
        -math.log(10000.0) * jnp.arange(half_width, dtype=jnp.float32) / half_width
    )
    angles = jnp.asarray(position).astype(jnp.float32)[..., None] * frequencies
    return jnp.concatenate([jnp.sin(angles), jnp.cos(angles)], axis=-1)


def up_to_lanes(count):
    return -(-count // LANES) * LANES


def window(first, count):
    start, stop = first // LANES * LANES, up_to_lanes(first + count)
    lane = lax.broadcasted_iota(jnp.int32, (1, stop - start), 1) + start
    return start, stop, (lane >= first) & (lane < first + count)


def head_scores(q_rows, kv_refs, head, head_dim):
    start, stop, own = window(head * head_dim, head_dim)
    q_head = jnp.where(own, q_rows[:, start:stop], jnp.zeros((), q_rows.dtype))
    return [
        lax.dot_general(
            q_head, kv[:, start:stop], (((1,), (1,)), ((), ())), preferred_element_type=jnp.float32
        )
        for kv in kv_refs
    ]


def row_max(scores):
    top = scores[0]
    for more in scores[1:]:
        top = jnp.maximum(top, more)
    return jnp.max(top, axis=-1, keepdims=True)


def weigh(scores, top, kv_refs, head, head_dim, width_win):
    factor = head_dim**-0.5 * math.log2(math.e)
    exps = [jnp.exp2((part - top) * factor) for part in scores]
    total = exps[0]
    for more in exps[1:]:
        total = total + more
    total = jnp.sum(total, axis=-1, keepdims=True)
    start, stop, own = window(width_win + head * head_dim, head_dim)
    mixed = None
    for part, kv in zip(exps, kv_refs):
        term = jnp.dot(
            part.astype(jnp.bfloat16), kv[:, start:stop], preferred_element_type=jnp.float32
        )
        mixed = term if mixed is None else mixed + term
    return total, jnp.where(own, mixed, 0.0), start, stop


def near_kernel(head_dim, width_win, q_ref, kv0_ref, kv1_ref, acc_ref, top_ref, sum_ref):
    base = width_win // LANES * LANES
    kv_refs = (kv0_ref, kv1_ref)
    q_rows = q_ref[...]
    acc_ref[...] = jnp.zeros_like(acc_ref)
    for head in range(width_win // head_dim):
        scores = head_scores(q_rows, kv_refs, head, head_dim)
        top = row_max(scores)
        total, mixed, start, stop = weigh(scores, top, kv_refs, head, head_dim, width_win)
        acc_ref[:, start - base : stop - base] += mixed
        top_ref[:, head : head + 1] = top
        sum_ref[:, head : head + 1] = total


def far_rows(head_dim, width_win, q_rows, kv_refs, acc, top_old, sum_old):
    base = width_win // LANES * LANES
    factor = head_dim**-0.5 * math.log2(math.e)
    tiles = [None] * ((2 * width_win - base) // LANES)
    for head in range(width_win // head_dim):
        scores = head_scores(q_rows, kv_refs, head, head_dim)
        before = top_old[:, head : head + 1]
        top = jnp.maximum(row_max(scores), before)
        total, mixed, start, stop = weigh(scores, top, kv_refs, head, head_dim, width_win)
        shrink = jnp.exp2((before - top) * factor)
        inverse = 1.0 / (total + sum_old[:, head : head + 1] * shrink)
        _, _, own = window(width_win + head * head_dim, head_dim)
        earlier = acc[:, start - base : stop - base] * jnp.where(own, shrink, 0.0)
        share = (mixed + earlier) * inverse
        for tile in range((stop - start) // LANES):
            at = (start - base) // LANES + tile
            piece = share[:, tile * LANES : (tile + 1) * LANES]
            tiles[at] = piece if tiles[at] is None else tiles[at] + piece
    return jnp.concatenate(tiles, axis=1).astype(jnp.bfloat16)


def spatial_finish(mixed, tokens, out_weight, mod, position):
    projected = jnp.dot(mixed, out_weight, preferred_element_type=jnp.float32)
    after = tokens.astype(jnp.float32) + mod[2:3] * projected
    temporal_in = normalize(after) * (1.0 + mod[4:5]) + mod[3:4] + position
    return after, temporal_in.astype(jnp.bfloat16)


def far_kernel(
    head_dim, width_win, q_ref, kv2_ref, kv3_ref, acc_ref, top_ref, sum_ref, tokens_ref,
    out_weight_ref, mod_ref, after_ref, temporal_ref,
):
    mixed = far_rows(
        head_dim, width_win, q_ref[...], (kv2_ref, kv3_ref), acc_ref, top_ref, sum_ref
    )
    after, temporal_in = spatial_finish(
        mixed, tokens_ref[...], out_weight_ref[...], mod_ref[...], mod_ref[6:7]
    )
    after_ref[...] = after
    temporal_ref[...] = temporal_in


def temporal_rows(head_dim, rows, weight, frames):
    width_win = weight.shape[2]
    count = rows.shape[0]
    pixels = count // frames
    q, k, v = (
        jnp.dot(rows, weight[part], preferred_element_type=jnp.float32).astype(jnp.bfloat16)
        for part in range(3)
    )
    feature = lax.broadcasted_iota(jnp.int32, (width_win, LANES), 0)
    head = lax.broadcasted_iota(jnp.int32, (width_win, LANES), 1)
    gather = ((feature >= head * head_dim) & (feature < (head + 1) * head_dim)).astype(jnp.bfloat16)
    feature = lax.broadcasted_iota(jnp.int32, (LANES, width_win), 1)
    head = lax.broadcasted_iota(jnp.int32, (LANES, width_win), 0)
    spread = ((feature >= head * head_dim) & (feature < (head + 1) * head_dim)).astype(jnp.bfloat16)
    k_wide, v_wide = k.astype(jnp.float32), v.astype(jnp.float32)
    outs = []
    for frame in range(frames):
        q_frame = q[frame * pixels : (frame + 1) * pixels].astype(jnp.float32)
        products = jnp.concatenate(
            [q_frame * k_wide[g * pixels : (g + 1) * pixels] for g in range(frames)], axis=0
        )
        high = products.astype(jnp.bfloat16)
        low = (products - high.astype(jnp.float32)).astype(jnp.bfloat16)
        scores = jnp.dot(high, gather, preferred_element_type=jnp.float32) + jnp.dot(
            low, gather, preferred_element_type=jnp.float32
        )
        scores = [scores[g * pixels : (g + 1) * pixels] * head_dim**-0.5 for g in range(frames)]
        top = functools.reduce(jnp.maximum, scores)
        exps = [jnp.exp(part - top) for part in scores]
        inverse = 1.0 / functools.reduce(jnp.add, exps)
        weights = jnp.concatenate([part * inverse for part in exps], axis=0).astype(jnp.bfloat16)
        spread_weights = jnp.dot(weights, spread, preferred_element_type=jnp.float32)
        terms = spread_weights * v_wide
        mixed = functools.reduce(
            jnp.add, [terms[g * pixels : (g + 1) * pixels] for g in range(frames)]
        )
        outs.append(mixed.astype(jnp.bfloat16))
    return outs


def temporal_kernel(head_dim, frames, rows_ref, weight_ref, out_ref):
    outs = temporal_rows(head_dim, rows_ref[...], weight_ref, frames)
    pixels = rows_ref.shape[0] // frames
    for frame in range(frames):
        out_ref[frame * pixels : (frame + 1) * pixels] = outs[frame]


def cost(flops, nbytes, exps=0):
    return pl.CostEstimate(flops=int(flops), bytes_accessed=int(nbytes), transcendentals=int(exps))


def per_device(
    tokens,
    stale_kv,
    mod_table,
    mod_mix,
    timestep,
    frame_order,
    spatial_qkv,
    spatial_out,
    temporal_qkv,
    temporal_out,
):
    devices = lax.axis_size("patch")
    dev_index = lax.axis_index("patch")
    frames = devices // 4
    frame_slot = dev_index // 4
    row_count, feature_width = tokens.shape
    width_win = spatial_out.shape[0]
    head_dim = feature_width // HEADS
    base = width_win // LANES * LANES
    q_width = up_to_lanes(width_win)
    v_width = 2 * width_win - base

    kv2 = swap_bit(stale_kv, "patch", 1)
    kv1 = swap_bit(stale_kv, "patch", 0)
    modulation = mod_table + mod_mix * sinusoid(timestep[0], feature_width)[None, :]
    frame_id = jnp.sum(jnp.where(jnp.arange(frames) == frame_slot, frame_order, 0))
    position = sinusoid(frame_id, feature_width)[None, :]
    mod = jnp.concatenate([modulation, position, jnp.zeros_like(position)], axis=0)
    tokens_wide = tokens.astype(jnp.float32)
    spatial_in = (normalize(tokens_wide) * (1.0 + modulation[1]) + modulation[0]).astype(
        jnp.bfloat16
    )
    fresh = jnp.einsum(
        "tr,jrd->jtd", spatial_in, spatial_qkv, preferred_element_type=jnp.float32
    ).astype(jnp.bfloat16)
    q = jnp.pad(fresh[0], ((0, 0), (0, q_width - width_win)))
    kv0 = jnp.concatenate([fresh[1], fresh[2]], axis=1)
    out_weight = jnp.pad(spatial_out, ((width_win - base, 0), (0, 0)))

    block = min(128, row_count)
    steps = row_count // block
    whole = lambda a: pl.BlockSpec(a.shape, lambda i: (0,) * a.ndim)
    rows_of = lambda width: pl.BlockSpec((block, width), lambda i: (i, 0))
    half_flops = 4 * row_count * (2 * row_count) * width_win
    acc, top, total = pl.pallas_call(
        functools.partial(near_kernel, head_dim, width_win),
        grid=(steps,),
        in_specs=[rows_of(q_width), whole(kv0), whole(kv1)],
        out_specs=[rows_of(v_width), rows_of(LANES), rows_of(LANES)],
        out_shape=[
            jax.ShapeDtypeStruct((row_count, v_width), jnp.float32),
            jax.ShapeDtypeStruct((row_count, LANES), jnp.float32),
            jax.ShapeDtypeStruct((row_count, LANES), jnp.float32),
        ],
        cost_estimate=cost(4 * half_flops, 6e6),
        name="near_attention",
    )(q, kv0, kv1)
    kv3 = swap_bit(kv2, "patch", 0)
    after_spatial, temporal_in = pl.pallas_call(
        functools.partial(far_kernel, head_dim, width_win),
        grid=(steps,),
        in_specs=[
            rows_of(q_width), whole(kv2), whole(kv3), rows_of(v_width), rows_of(LANES),
            rows_of(LANES), rows_of(feature_width), whole(out_weight), whole(mod),
        ],
        out_specs=[rows_of(feature_width), rows_of(feature_width)],
        out_shape=[
            jax.ShapeDtypeStruct((row_count, feature_width), jnp.float32),
            jax.ShapeDtypeStruct((row_count, feature_width), jnp.bfloat16),
        ],
        cost_estimate=cost(4 * half_flops, 1e7),
        name="far_attention",
    )(q, kv2, kv3, acc, top, total, tokens, out_weight, mod)

    pixels = row_count // frames
    groups = [[4 * f + c for f in range(frames)] for c in range(4)]
    exchange = functools.partial(
        lax.all_to_all, axis_name="patch", split_axis=0, concat_axis=0,
        axis_index_groups=groups, tiled=True,
    )
    arranged = exchange(temporal_in)
    mixed = pl.pallas_call(
        functools.partial(temporal_kernel, head_dim, frames),
        in_specs=[pl.BlockSpec(memory_space=pltpu.VMEM)] * 2,
        out_specs=pl.BlockSpec(memory_space=pltpu.VMEM),
        out_shape=jax.ShapeDtypeStruct((row_count, width_win), jnp.bfloat16),
        cost_estimate=cost(6 * row_count * feature_width * width_win, 6e6),
        compiler_params=pltpu.CompilerParams(vmem_limit_bytes=60 * 1024 * 1024),
        name="temporal_attention",
    )(arranged, temporal_qkv)
    temporal_mixed = exchange(mixed)
    projected = jnp.dot(temporal_mixed, temporal_out, preferred_element_type=jnp.float32)
    return after_spatial + modulation[5] * projected


def solution(mesh):
    return jax.shard_map(
        per_device,
        mesh=mesh,
        in_specs=(
            P(("groups", "patch"), None),
            P(("groups", "patch"), None),
            P(),
            P(),
            P("groups"),
            P("groups"),
            P(),
            P(),
            P(),
            P(),
        ),
        out_specs=P(("groups", "patch"), None),
        check_vma=False,
    )
```

```python
import functools
import math

import jax
import jax.numpy as jnp
from jax import lax
from jax.experimental import pallas as pl
from jax.experimental.pallas import tpu as pltpu
from jax.sharding import PartitionSpec as P

HEADS = 16
LANES = 128

epsilon = 1e-06


def normalize(activations):
    row_mean = jnp.mean(activations, axis=-1, keepdims=True)
    centered = activations - row_mean
    variance = jnp.mean(centered * centered, axis=-1, keepdims=True)
    return centered * lax.rsqrt(variance + epsilon)


def sinusoid(position, feature_width):
    half_width = feature_width // 2
    frequencies = jnp.exp(
        -math.log(10000.0) * jnp.arange(half_width, dtype=jnp.float32) / half_width
    )
    angles = jnp.asarray(position).astype(jnp.float32)[..., None] * frequencies
    return jnp.concatenate([jnp.sin(angles), jnp.cos(angles)], axis=-1)


def up_to_lanes(count):
    return -(-count // LANES) * LANES


def window(first, count):
    start, stop = first // LANES * LANES, up_to_lanes(first + count)
    lane = lax.broadcasted_iota(jnp.int32, (1, stop - start), 1) + start
    return start, stop, (lane >= first) & (lane < first + count)


def head_scores(q_rows, kv_refs, head, head_dim):
    start, stop, own = window(head * head_dim, head_dim)
    q_head = jnp.where(own, q_rows[:, start:stop], jnp.zeros((), q_rows.dtype))
    return [
        lax.dot_general(
            q_head, kv[:, start:stop], (((1,), (1,)), ((), ())), preferred_element_type=jnp.float32
        )
        for kv in kv_refs
    ]


def row_max(scores):
    top = scores[0]
    for more in scores[1:]:
        top = jnp.maximum(top, more)
    return jnp.max(top, axis=-1, keepdims=True)


def weigh(scores, top, kv_refs, head, head_dim, width_win):
    factor = head_dim**-0.5 * math.log2(math.e)
    exps = [jnp.exp2((part - top) * factor) for part in scores]
    total = exps[0]
    for more in exps[1:]:
        total = total + more
    total = jnp.sum(total, axis=-1, keepdims=True)
    start, stop, own = window(width_win + head * head_dim, head_dim)
    mixed = None
    for part, kv in zip(exps, kv_refs):
        term = jnp.dot(
            part.astype(jnp.bfloat16), kv[:, start:stop], preferred_element_type=jnp.float32
        )
        mixed = term if mixed is None else mixed + term
    return total, jnp.where(own, mixed, 0.0), start, stop


def near_rows(head_dim, width_win, q_rows, kv_refs, acc, top_ref, sum_ref, at, count):
    base = width_win // LANES * LANES
    heads = width_win // head_dim
    here = pl.ds(at, count)
    acc[here] = jnp.zeros((count,) + acc.shape[1:], acc.dtype)
    scores = head_scores(q_rows, kv_refs, 0, head_dim)
    for head in range(heads):
        later = head_scores(q_rows, kv_refs, head + 1, head_dim) if head + 1 < heads else None
        top = row_max(scores)
        total, mixed, start, stop = weigh(scores, top, kv_refs, head, head_dim, width_win)
        acc[here, :, start - base : stop - base] += mixed.reshape(count, -1, stop - start)
        top_ref[here, :, head : head + 1] = top.reshape(count, -1, 1)
        sum_ref[here, :, head : head + 1] = total.reshape(count, -1, 1)
        scores = later


def far_rows(head_dim, width_win, q_rows, kv_refs, acc, top_old, sum_old):
    base = width_win // LANES * LANES
    factor = head_dim**-0.5 * math.log2(math.e)
    tiles = [None] * ((2 * width_win - base) // LANES)
    heads = width_win // head_dim
    scores = head_scores(q_rows, kv_refs, 0, head_dim)
    for head in range(heads):
        later = head_scores(q_rows, kv_refs, head + 1, head_dim) if head + 1 < heads else None
        before = top_old[:, head : head + 1]
        top = jnp.maximum(row_max(scores), before)
        total, mixed, start, stop = weigh(scores, top, kv_refs, head, head_dim, width_win)
        shrink = jnp.exp2((before - top) * factor)
        inverse = 1.0 / (total + sum_old[:, head : head + 1] * shrink)
        _, _, own = window(width_win + head * head_dim, head_dim)
        earlier = acc[:, start - base : stop - base] * jnp.where(own, shrink, 0.0)
        share = (mixed + earlier) * inverse
        for tile in range((stop - start) // LANES):
            at = (start - base) // LANES + tile
            piece = share[:, tile * LANES : (tile + 1) * LANES]
            tiles[at] = piece if tiles[at] is None else tiles[at] + piece
        scores = later
    return jnp.concatenate(tiles, axis=1).astype(jnp.bfloat16)


def spatial_finish(mixed, tokens, out_weight, mod, position):
    projected = jnp.dot(mixed, out_weight, preferred_element_type=jnp.float32)
    after = tokens.astype(jnp.float32) + mod[2:3] * projected
    temporal_in = normalize(after) * (1.0 + mod[4:5]) + mod[3:4] + position
    return after, temporal_in.astype(jnp.bfloat16)


def times_transposed(rows, weight):
    return lax.dot_general(
        rows, weight, (((1,), (1,)), ((), ())), preferred_element_type=jnp.float32
    )


def temporal_rows(head_dim, rows, weight, frames):
    width_win = weight.shape[0] // 3
    count = rows.shape[0]
    pixels = count // frames
    q, k, v = (
        times_transposed(rows, weight[part * width_win : (part + 1) * width_win]).astype(jnp.bfloat16)
        for part in range(3)
    )
    feature = lax.broadcasted_iota(jnp.int32, (width_win, LANES), 0)
    head = lax.broadcasted_iota(jnp.int32, (width_win, LANES), 1)
    gather = ((feature >= head * head_dim) & (feature < (head + 1) * head_dim)).astype(jnp.bfloat16)
    feature = lax.broadcasted_iota(jnp.int32, (LANES, width_win), 1)
    head = lax.broadcasted_iota(jnp.int32, (LANES, width_win), 0)
    spread = ((feature >= head * head_dim) & (feature < (head + 1) * head_dim)).astype(jnp.bfloat16)
    k_wide, v_wide = k.astype(jnp.float32), v.astype(jnp.float32)
    outs = []
    for frame in range(frames):
        q_frame = q[frame * pixels : (frame + 1) * pixels].astype(jnp.float32)
        products = jnp.concatenate(
            [q_frame * k_wide[g * pixels : (g + 1) * pixels] for g in range(frames)], axis=0
        )
        high = products.astype(jnp.bfloat16)
        low = (products - high.astype(jnp.float32)).astype(jnp.bfloat16)
        scores = jnp.dot(high, gather, preferred_element_type=jnp.float32) + jnp.dot(
            low, gather, preferred_element_type=jnp.float32
        )
        scores = [scores[g * pixels : (g + 1) * pixels] * head_dim**-0.5 for g in range(frames)]
        top = functools.reduce(jnp.maximum, scores)
        exps = [jnp.exp(part - top) for part in scores]
        inverse = 1.0 / functools.reduce(jnp.add, exps)
        weights = jnp.concatenate([part * inverse for part in exps], axis=0).astype(jnp.bfloat16)
        spread_weights = jnp.dot(weights, spread, preferred_element_type=jnp.float32)
        terms = spread_weights * v_wide
        mixed = functools.reduce(
            jnp.add, [terms[g * pixels : (g + 1) * pixels] for g in range(frames)]
        )
        outs.append(mixed.astype(jnp.bfloat16))
    return outs


def block_kernel(
    head_dim, tokens_hbm, stale_hbm, spatial_w_hbm, spatial_o_hbm, temporal_w_hbm, temporal_o_hbm,
    mod_ref, out_ref, tokens, kv0, kv1, kv2, kv3, q, spatial_w, spatial_o, temporal_w, temporal_o,
    acc, top, total, leaving, arriving, mixed_out, mixed_in, load_sem, kv_send, kv_recv, in_send,
    in_recv, back_send, back_recv, own_sem,
):
    chunks, frames, pixels, _ = leaving.shape
    rows = frames * pixels
    width_win = temporal_o.shape[0]
    base = width_win // LANES * LANES
    device = lax.axis_index("patch")
    slot, quarter = device // 4, device % 4

    def flip(mask):
        bit = device // mask % 2
        return device + mask - 2 * mask * bit

    def peer(step):
        other = (slot + step) % frames
        return other, other * 4 + quarter

    loads = [
        pltpu.make_async_copy(source, target, load_sem.at[at])
        for at, (source, target) in enumerate(
            [
                (tokens_hbm, tokens),
                (spatial_w_hbm, spatial_w),
                (spatial_o_hbm, spatial_o.at[width_win - base :]),
                (temporal_w_hbm, temporal_w),
                (temporal_o_hbm, temporal_o),
            ]
        )
    ]
    for load in loads:
        load.start()

    barrier = pltpu.get_barrier_semaphore()
    others = [flip(2), flip(1)] + [peer(step)[1] for step in range(1, frames)]
    for other in others:
        pl.semaphore_signal(
            barrier, inc=1, device_id={"patch": other}, device_id_type=pl.DeviceIdType.MESH
        )
    pl.semaphore_wait(barrier, len(others))

    def remote(source, target, send, recv, other):
        return pltpu.make_async_remote_copy(
            src_ref=source, dst_ref=target, send_sem=send, recv_sem=recv,
            device_id={"patch": other}, device_id_type=pl.DeviceIdType.MESH,
        )

    across = remote(stale_hbm, kv2, kv_send.at[0], kv_recv.at[0], flip(2))
    beside = remote(stale_hbm, kv1, kv_send.at[1], kv_recv.at[1], flip(1))
    onward = remote(kv2, kv3, kv_send.at[2], kv_recv.at[2], flip(1))
    across.start()
    beside.start()

    spatial_o[: width_win - base] = jnp.zeros((width_win - base, spatial_o.shape[1]), jnp.bfloat16)
    loads[0].wait()
    loads[1].wait()

    def project(c, carry):
        wide = tokens[c].astype(jnp.float32)
        spatial_in = (normalize(wide) * (1.0 + mod_ref[1:2]) + mod_ref[0:1]).astype(jnp.bfloat16)
        here = pl.ds(pl.multiple_of(c * rows, rows), rows)
        fresh_q, fresh_k, fresh_v = (
            times_transposed(spatial_in, spatial_w[part * width_win : (part + 1) * width_win])
            .astype(jnp.bfloat16)
            for part in range(3)
        )
        q[c, :, :width_win] = fresh_q
        q[c, :, width_win:] = jnp.zeros((rows, q.shape[2] - width_win), jnp.bfloat16)
        kv0[here, :width_win] = fresh_k
        kv0[here, width_win:] = fresh_v
        return carry

    lax.fori_loop(0, chunks, project, 0)
    beside.wait_recv()

    near_count = 2 if chunks % 2 == 0 and rows <= 128 else 1

    def near(block, carry):
        at = block * near_count
        q_rows = q[pl.ds(at, near_count)].reshape(near_count * rows, q.shape[2])
        near_rows(head_dim, width_win, q_rows, (kv0, kv1), acc, top, total, at, near_count)
        return carry

    lax.fori_loop(0, chunks // near_count, near, 0)
    across.wait_recv()
    onward.start()
    loads[2].wait()
    loads[3].wait()
    loads[4].wait()
    onward.wait_recv()

    def inward(c, step):
        other, target = peer(step)
        return other, remote(
            leaving.at[c, other], arriving.at[c, slot], in_send.at[c, step], in_recv.at[c, step],
            target,
        )

    def backward(c, step):
        other, target = peer(step)
        return remote(
            mixed_out.at[c, other], mixed_in.at[c, slot], back_send.at[c, step],
            back_recv.at[c, step], target,
        )

    def keep(c):
        return pltpu.make_async_copy(leaving.at[c, slot], arriving.at[c, slot], own_sem.at[0, c])

    def keep_back(c):
        return pltpu.make_async_copy(mixed_out.at[c, slot], mixed_in.at[c, slot], own_sem.at[1, c])

    def far(c):
        mixed = far_rows(
            head_dim, width_win, q[c], (kv2, kv3), acc.at[c], top.at[c], total.at[c]
        )
        after, temporal_in = spatial_finish(
            mixed, tokens[c], spatial_o[...], mod_ref, mod_ref[6:7]
        )
        out_ref[c] = after
        leaving[c] = temporal_in.reshape(frames, pixels, temporal_in.shape[1])
        for step in range(1, frames):
            inward(c, step)[1].start()
        keep(c).start()

    def temporal(c):
        for step in range(1, frames):
            inward(c, step)[1].wait_recv()
        keep(c).wait()
        flat = arriving[c].reshape(rows, arriving.shape[3])
        for frame, mixed in enumerate(temporal_rows(head_dim, flat, temporal_w, frames)):
            mixed_out[c, frame] = mixed
        for step in range(1, frames):
            backward(c, step).start()
        keep_back(c).start()

    lag = min(2, chunks - 1)

    def first(c, carry):
        far(c)

        @pl.when(c >= lag)
        def _():
            temporal(c - lag)

        return carry

    def second(c, carry):
        temporal(c)
        return carry

    def third(c, carry):
        for step in range(1, frames):
            backward(c, step).wait_recv()
        keep_back(c).wait()
        mixed = mixed_in[c].reshape(rows, width_win)
        projected = jnp.dot(mixed, temporal_o[...], preferred_element_type=jnp.float32)
        out_ref[c] = out_ref[c] + mod_ref[5:6] * projected
        return carry

    lax.fori_loop(0, chunks, first, 0)
    lax.fori_loop(chunks - lag, chunks, second, 0)
    lax.fori_loop(0, chunks, third, 0)

    def drain(c, carry):
        for step in range(1, frames):
            inward(c, step)[1].wait_send()
            backward(c, step).wait_send()
        return carry

    lax.fori_loop(0, chunks, drain, 0)
    for copy in (across, beside, onward):
        copy.wait_send()


def per_device(
    tokens,
    stale_kv,
    mod_table,
    mod_mix,
    timestep,
    frame_order,
    spatial_qkv,
    spatial_out,
    temporal_qkv,
    temporal_out,
):
    devices = lax.axis_size("patch")
    dev_index = lax.axis_index("patch")
    frames = devices // 4
    frame_slot = dev_index // 4
    row_count, feature_width = tokens.shape
    width_win = spatial_out.shape[0]
    head_dim = feature_width // HEADS
    base = width_win // LANES * LANES
    q_width = up_to_lanes(width_win)
    v_width = 2 * width_win - base

    modulation = mod_table + mod_mix * sinusoid(timestep[0], feature_width)[None, :]
    frame_id = jnp.sum(jnp.where(jnp.arange(frames) == frame_slot, frame_order, 0))
    position = sinusoid(frame_id, feature_width)[None, :]
    mod = jnp.concatenate([modulation, position, jnp.zeros_like(position)], axis=0)
    chunks = max(1, min(4, row_count // (16 * frames)))
    rows = row_count // chunks
    pixels = rows // frames
    transposed = lambda w: jnp.swapaxes(w, 1, 2).reshape(3 * width_win, feature_width)
    flat = (row_count, feature_width)
    chunked = (chunks, rows, feature_width)
    exchanged = (chunks, frames, pixels)
    anywhere = pl.BlockSpec(memory_space=pl.ANY)
    bf16, f32 = jnp.bfloat16, jnp.float32
    out = pl.pallas_call(
        functools.partial(block_kernel, head_dim),
        in_specs=[anywhere] * 6 + [pl.BlockSpec(memory_space=pltpu.VMEM)],
        out_specs=pl.BlockSpec(memory_space=pltpu.VMEM),
        out_shape=jax.ShapeDtypeStruct(chunked, f32),
        scratch_shapes=[
            pltpu.VMEM(chunked, bf16),
            pltpu.VMEM(flat, bf16),
            pltpu.VMEM(flat, bf16),
            pltpu.VMEM(flat, bf16),
            pltpu.VMEM(flat, bf16),
            pltpu.VMEM((chunks, rows, q_width), bf16),
            pltpu.VMEM((3 * width_win, feature_width), bf16),
            pltpu.VMEM((v_width, feature_width), bf16),
            pltpu.VMEM((3 * width_win, feature_width), bf16),
            pltpu.VMEM((width_win, feature_width), bf16),
            pltpu.VMEM((chunks, rows, v_width), f32),
            pltpu.VMEM((chunks, rows, LANES), f32),
            pltpu.VMEM((chunks, rows, LANES), f32),
            pltpu.VMEM(exchanged + (feature_width,), bf16),
            pltpu.VMEM(exchanged + (feature_width,), bf16),
            pltpu.VMEM(exchanged + (width_win,), bf16),
            pltpu.VMEM(exchanged + (width_win,), bf16),
            pltpu.SemaphoreType.DMA((5,)),
            pltpu.SemaphoreType.DMA((3,)),
            pltpu.SemaphoreType.DMA((3,)),
            pltpu.SemaphoreType.DMA((chunks, frames)),
            pltpu.SemaphoreType.DMA((chunks, frames)),
            pltpu.SemaphoreType.DMA((chunks, frames)),
            pltpu.SemaphoreType.DMA((chunks, frames)),
            pltpu.SemaphoreType.DMA((2, chunks)),
        ],
        compiler_params=pltpu.CompilerParams(
            collective_id=0, has_side_effects=True, vmem_limit_bytes=60 * 1024 * 1024
        ),
        name="denoising_block",
    )(
        tokens.reshape(chunked), stale_kv, transposed(spatial_qkv), spatial_out,
        transposed(temporal_qkv), temporal_out, mod,
    )
    return out.reshape(flat)


def solution(mesh):
    return jax.shard_map(
        per_device,
        mesh=mesh,
        in_specs=(
            P(("groups", "patch"), None),
            P(("groups", "patch"), None),
            P(),
            P(),
            P("groups"),
            P("groups"),
            P(),
            P(),
            P(),
            P(),
        ),
        out_specs=P(("groups", "patch"), None),
        check_vma=False,
    )
```

```python
import functools
import math

import jax
import jax.numpy as jnp
from jax import lax
from jax.experimental import pallas as pl
from jax.experimental.pallas import tpu as pltpu
from jax.sharding import PartitionSpec as P

HEADS = 16
LANES = 128

epsilon = 1e-06


def normalize(activations):
    row_mean = jnp.mean(activations, axis=-1, keepdims=True)
    centered = activations - row_mean
    variance = jnp.mean(centered * centered, axis=-1, keepdims=True)
    return centered * lax.rsqrt(variance + epsilon)


def sinusoid(position, feature_width):
    half_width = feature_width // 2
    frequencies = jnp.exp(
        -math.log(10000.0) * jnp.arange(half_width, dtype=jnp.float32) / half_width
    )
    angles = jnp.asarray(position).astype(jnp.float32)[..., None] * frequencies
    return jnp.concatenate([jnp.sin(angles), jnp.cos(angles)], axis=-1)


def up_to_lanes(count):
    return -(-count // LANES) * LANES


def window(first, count):
    start, stop = first // LANES * LANES, up_to_lanes(first + count)
    lane = lax.broadcasted_iota(jnp.int32, (1, stop - start), 1) + start
    return start, stop, (lane >= first) & (lane < first + count)


def head_scores(q_rows, kv_refs, head, head_dim):
    start, stop, own = window(head * head_dim, head_dim)
    q_head = jnp.where(own, q_rows[:, start:stop], jnp.zeros((), q_rows.dtype))
    return [
        lax.dot_general(
            q_head, kv[:, start:stop], (((1,), (1,)), ((), ())), preferred_element_type=jnp.float32
        )
        for kv in kv_refs
    ]


def row_max(scores):
    top = scores[0]
    for more in scores[1:]:
        top = jnp.maximum(top, more)
    return jnp.max(top, axis=-1, keepdims=True)


def weigh(scores, top, kv_refs, head, head_dim, width_win):
    factor = head_dim**-0.5 * math.log2(math.e)
    exps = [jnp.exp2((part - top) * factor) for part in scores]
    total = exps[0]
    for more in exps[1:]:
        total = total + more
    total = jnp.sum(total, axis=-1, keepdims=True)
    start, stop, own = window(width_win + head * head_dim, head_dim)
    mixed = None
    for part, kv in zip(exps, kv_refs):
        term = jnp.dot(
            part.astype(jnp.bfloat16), kv[:, start:stop], preferred_element_type=jnp.float32
        )
        mixed = term if mixed is None else mixed + term
    return total, jnp.where(own, mixed, 0.0), start, stop


def near_rows(head_dim, width_win, q_rows, kv_refs, acc, top_ref, sum_ref, at, count):
    base = width_win // LANES * LANES
    heads = width_win // head_dim
    here = pl.ds(at, count)
    acc[here] = jnp.zeros((count,) + acc.shape[1:], acc.dtype)
    scores = head_scores(q_rows, kv_refs, 0, head_dim)
    for head in range(heads):
        later = head_scores(q_rows, kv_refs, head + 1, head_dim) if head + 1 < heads else None
        top = row_max(scores)
        total, mixed, start, stop = weigh(scores, top, kv_refs, head, head_dim, width_win)
        acc[here, :, start - base : stop - base] += mixed.reshape(count, -1, stop - start)
        top_ref[here, :, head : head + 1] = top.reshape(count, -1, 1)
        sum_ref[here, :, head : head + 1] = total.reshape(count, -1, 1)
        scores = later


def far_message(head_dim, width_win, q_rows, kv_refs):
    base = width_win // LANES * LANES
    heads = width_win // head_dim
    tiles = [None] * ((2 * width_win - base) // LANES)
    lane = lax.broadcasted_iota(jnp.int32, (1, LANES), 1)
    stats = jnp.zeros((q_rows.shape[0], LANES), jnp.float32)
    scores = head_scores(q_rows, kv_refs, 0, head_dim)
    for head in range(heads):
        later = head_scores(q_rows, kv_refs, head + 1, head_dim) if head + 1 < heads else None
        top = row_max(scores)
        total, mixed, start, stop = weigh(scores, top, kv_refs, head, head_dim, width_win)
        own = lane % heads == head
        stats = jnp.where(own & (lane < 3 * heads), top, stats)
        stats = jnp.where(own & (lane >= 3 * heads) & (lane < 6 * heads), total, stats)
        for tile in range((stop - start) // LANES):
            at = (start - base) // LANES + tile
            piece = mixed[:, tile * LANES : (tile + 1) * LANES]
            tiles[at] = piece if tiles[at] is None else tiles[at] + piece
        scores = later
    high = stats.astype(jnp.bfloat16).astype(jnp.float32)
    middle = (stats - high).astype(jnp.bfloat16).astype(jnp.float32)
    low = stats - high - middle
    part = lane // heads % 3
    split = jnp.where(part == 0, high, jnp.where(part == 1, middle, low))
    tiles[0] = jnp.where(lane < 6 * heads, split, tiles[0])
    return jnp.concatenate(tiles, axis=1).astype(jnp.bfloat16)


def join(head_dim, width_win, message, acc, top, total):
    base = width_win // LANES * LANES
    heads = width_win // head_dim
    factor = head_dim**-0.5 * math.log2(math.e)
    source = lax.broadcasted_iota(jnp.int32, (LANES, LANES), 0)
    target = lax.broadcasted_iota(jnp.int32, (LANES, LANES), 1)
    wanted = jnp.where(source < 3 * heads, source % heads, heads + source % heads)
    picks = ((source < 6 * heads) & (target == wanted)).astype(jnp.bfloat16)
    stats = jnp.dot(message[:, :LANES], picks, preferred_element_type=jnp.float32)
    tiles = [None] * ((2 * width_win - base) // LANES)
    for head in range(heads):
        near_top, far_top = top[:, head : head + 1], stats[:, head : head + 1]
        best = jnp.maximum(near_top, far_top)
        near_part = jnp.exp2((near_top - best) * factor)
        far_part = jnp.exp2((far_top - best) * factor)
        far_sum = stats[:, heads + head : heads + head + 1]
        inverse = 1.0 / (total[:, head : head + 1] * near_part + far_sum * far_part)
        start, stop, own = window(width_win + head * head_dim, head_dim)
        here = slice(start - base, stop - base)
        near_share = acc[:, here] * jnp.where(own, near_part * inverse, 0.0)
        far_share = message[:, here].astype(jnp.float32) * jnp.where(own, far_part * inverse, 0.0)
        share = near_share + far_share
        for tile in range((stop - start) // LANES):
            at = (start - base) // LANES + tile
            piece = share[:, tile * LANES : (tile + 1) * LANES]
            tiles[at] = piece if tiles[at] is None else tiles[at] + piece
    return jnp.concatenate(tiles, axis=1).astype(jnp.bfloat16)


def spatial_finish(mixed, tokens, out_weight, mod, position):
    projected = jnp.dot(mixed, out_weight, preferred_element_type=jnp.float32)
    after = tokens.astype(jnp.float32) + mod[2:3] * projected
    temporal_in = normalize(after) * (1.0 + mod[4:5]) + mod[3:4] + position
    return after, temporal_in.astype(jnp.bfloat16)


def times_transposed(rows, weight):
    return lax.dot_general(
        rows, weight, (((1,), (1,)), ((), ())), preferred_element_type=jnp.float32
    )


def temporal_rows(head_dim, rows, weight, frames):
    width_win = weight.shape[0] // 3
    count = rows.shape[0]
    pixels = count // frames
    q, k, v = (
        times_transposed(rows, weight[part * width_win : (part + 1) * width_win]).astype(jnp.bfloat16)
        for part in range(3)
    )
    feature = lax.broadcasted_iota(jnp.int32, (width_win, LANES), 0)
    head = lax.broadcasted_iota(jnp.int32, (width_win, LANES), 1)
    gather = ((feature >= head * head_dim) & (feature < (head + 1) * head_dim)).astype(jnp.bfloat16)
    feature = lax.broadcasted_iota(jnp.int32, (LANES, width_win), 1)
    head = lax.broadcasted_iota(jnp.int32, (LANES, width_win), 0)
    spread = ((feature >= head * head_dim) & (feature < (head + 1) * head_dim)).astype(jnp.bfloat16)
    k_wide, v_wide = k.astype(jnp.float32), v.astype(jnp.float32)
    outs = []
    for frame in range(frames):
        q_frame = q[frame * pixels : (frame + 1) * pixels].astype(jnp.float32)
        products = jnp.concatenate(
            [q_frame * k_wide[g * pixels : (g + 1) * pixels] for g in range(frames)], axis=0
        )
        high = products.astype(jnp.bfloat16)
        low = (products - high.astype(jnp.float32)).astype(jnp.bfloat16)
        scores = jnp.dot(high, gather, preferred_element_type=jnp.float32) + jnp.dot(
            low, gather, preferred_element_type=jnp.float32
        )
        scores = [scores[g * pixels : (g + 1) * pixels] * head_dim**-0.5 for g in range(frames)]
        top = functools.reduce(jnp.maximum, scores)
        exps = [jnp.exp(part - top) for part in scores]
        inverse = 1.0 / functools.reduce(jnp.add, exps)
        weights = jnp.concatenate([part * inverse for part in exps], axis=0).astype(jnp.bfloat16)
        spread_weights = jnp.dot(weights, spread, preferred_element_type=jnp.float32)
        terms = spread_weights * v_wide
        mixed = functools.reduce(
            jnp.add, [terms[g * pixels : (g + 1) * pixels] for g in range(frames)]
        )
        outs.append(mixed.astype(jnp.bfloat16))
    return outs


def block_kernel(
    head_dim, tokens_hbm, stale_hbm, spatial_w_hbm, spatial_o_hbm, temporal_w_hbm, temporal_o_hbm,
    mod_ref, out_ref, tokens, kv0, kv1, stale, q, q_in, far_out, far_in, spatial_w, spatial_o, temporal_w, temporal_o,
    acc, top, total, leaving, arriving, mixed_out, mixed_in, load_sem, kv_send, kv_recv, far_send, far_recv, in_send,
    in_recv, back_send, back_recv, own_sem,
):
    chunks, frames, pixels, _ = leaving.shape
    rows = frames * pixels
    width_win = temporal_o.shape[0]
    base = width_win // LANES * LANES
    device = lax.axis_index("patch")
    slot, quarter = device // 4, device % 4

    def flip(mask):
        bit = device // mask % 2
        return device + mask - 2 * mask * bit

    def peer(step):
        other = (slot + step) % frames
        return other, other * 4 + quarter

    loads = [
        pltpu.make_async_copy(source, target, load_sem.at[at])
        for at, (source, target) in enumerate(
            [
                (tokens_hbm, tokens),
                (spatial_w_hbm, spatial_w),
                (stale_hbm, stale),
                (spatial_o_hbm, spatial_o.at[width_win - base :]),
                (temporal_w_hbm, temporal_w),
                (temporal_o_hbm, temporal_o),
            ]
        )
    ]
    for load in loads:
        load.start()

    barrier = pltpu.get_barrier_semaphore()
    others = [flip(2), flip(1)] + [peer(step)[1] for step in range(1, frames)]
    for other in others:
        pl.semaphore_signal(
            barrier, inc=1, device_id={"patch": other}, device_id_type=pl.DeviceIdType.MESH
        )
    pl.semaphore_wait(barrier, len(others))

    def remote(source, target, send, recv, other):
        return pltpu.make_async_remote_copy(
            src_ref=source, dst_ref=target, send_sem=send, recv_sem=recv,
            device_id={"patch": other}, device_id_type=pl.DeviceIdType.MESH,
        )

    beside = remote(stale_hbm, kv1, kv_send.at[0], kv_recv.at[0], flip(1))
    beside.start()

    def ask(c):
        return remote(q.at[c], q_in.at[c], far_send.at[0, c], far_recv.at[0, c], flip(2))

    def answer(c):
        return remote(far_out.at[c], far_in.at[c], far_send.at[1, c], far_recv.at[1, c], flip(2))

    spatial_o[: width_win - base] = jnp.zeros((width_win - base, spatial_o.shape[1]), jnp.bfloat16)
    loads[0].wait()
    loads[1].wait()

    def project(c, carry):
        wide = tokens[c].astype(jnp.float32)
        spatial_in = (normalize(wide) * (1.0 + mod_ref[1:2]) + mod_ref[0:1]).astype(jnp.bfloat16)
        here = pl.ds(pl.multiple_of(c * rows, rows), rows)
        fresh_q, fresh_k, fresh_v = (
            times_transposed(spatial_in, spatial_w[part * width_win : (part + 1) * width_win])
            .astype(jnp.bfloat16)
            for part in range(3)
        )
        q[c, :, :width_win] = fresh_q
        q[c, :, width_win:] = jnp.zeros((rows, q.shape[2] - width_win), jnp.bfloat16)
        kv0[here, :width_win] = fresh_k
        kv0[here, width_win:] = fresh_v
        ask(c).start()
        return carry

    lax.fori_loop(0, chunks, project, 0)
    for load in loads[2:]:
        load.wait()
    beside.wait_recv()

    def serve(c):
        ask(c).wait_recv()
        far_out[c] = far_message(head_dim, width_win, q_in[c], (stale, kv1))
        answer(c).start()

    def inward(c, step):
        other, target = peer(step)
        return other, remote(
            leaving.at[c, other], arriving.at[c, slot], in_send.at[c, step], in_recv.at[c, step],
            target,
        )

    def backward(c, step):
        other, target = peer(step)
        return remote(
            mixed_out.at[c, other], mixed_in.at[c, slot], back_send.at[c, step],
            back_recv.at[c, step], target,
        )

    def keep(c):
        return pltpu.make_async_copy(leaving.at[c, slot], arriving.at[c, slot], own_sem.at[0, c])

    def keep_back(c):
        return pltpu.make_async_copy(mixed_out.at[c, slot], mixed_in.at[c, slot], own_sem.at[1, c])

    def own(c):
        near_rows(head_dim, width_win, q[c], (kv0, kv1), acc, top, total, c, 1)
        answer(c).wait_recv()
        mixed = join(head_dim, width_win, far_in[c], acc.at[c], top.at[c], total.at[c])
        after, temporal_in = spatial_finish(
            mixed, tokens[c], spatial_o[...], mod_ref, mod_ref[6:7]
        )
        out_ref[c] = after
        leaving[c] = temporal_in.reshape(frames, pixels, temporal_in.shape[1])
        for step in range(1, frames):
            inward(c, step)[1].start()
        keep(c).start()

    def temporal(c):
        for step in range(1, frames):
            inward(c, step)[1].wait_recv()
        keep(c).wait()
        flat = arriving[c].reshape(rows, arriving.shape[3])
        for frame, mixed in enumerate(temporal_rows(head_dim, flat, temporal_w, frames)):
            mixed_out[c, frame] = mixed
        for step in range(1, frames):
            backward(c, step).start()
        keep_back(c).start()

    def stage(k, carry):
        @pl.when(k < chunks)
        def _():
            serve(k)

        @pl.when((k >= 1) & (k <= chunks))
        def _():
            own(k - 1)

        @pl.when(k >= 2)
        def _():
            temporal(k - 2)

        return carry

    def third(c, carry):
        for step in range(1, frames):
            backward(c, step).wait_recv()
        keep_back(c).wait()
        mixed = mixed_in[c].reshape(rows, width_win)
        projected = jnp.dot(mixed, temporal_o[...], preferred_element_type=jnp.float32)
        out_ref[c] = out_ref[c] + mod_ref[5:6] * projected
        return carry

    lax.fori_loop(0, chunks + 2, stage, 0)
    lax.fori_loop(0, chunks, third, 0)

    def drain(c, carry):
        ask(c).wait_send()
        answer(c).wait_send()
        for step in range(1, frames):
            inward(c, step)[1].wait_send()
            backward(c, step).wait_send()
        return carry

    lax.fori_loop(0, chunks, drain, 0)
    beside.wait_send()


def per_device(
    tokens,
    stale_kv,
    mod_table,
    mod_mix,
    timestep,
    frame_order,
    spatial_qkv,
    spatial_out,
    temporal_qkv,
    temporal_out,
):
    devices = lax.axis_size("patch")
    dev_index = lax.axis_index("patch")
    frames = devices // 4
    frame_slot = dev_index // 4
    row_count, feature_width = tokens.shape
    width_win = spatial_out.shape[0]
    head_dim = feature_width // HEADS
    base = width_win // LANES * LANES
    q_width = up_to_lanes(width_win)
    v_width = 2 * width_win - base

    modulation = mod_table + mod_mix * sinusoid(timestep[0], feature_width)[None, :]
    frame_id = jnp.sum(jnp.where(jnp.arange(frames) == frame_slot, frame_order, 0))
    position = sinusoid(frame_id, feature_width)[None, :]
    mod = jnp.concatenate([modulation, position, jnp.zeros_like(position)], axis=0)
    chunks = max(1, min(4, row_count // (16 * frames)))
    rows = row_count // chunks
    pixels = rows // frames
    transposed = lambda w: jnp.swapaxes(w, 1, 2).reshape(3 * width_win, feature_width)
    flat = (row_count, feature_width)
    chunked = (chunks, rows, feature_width)
    exchanged = (chunks, frames, pixels)
    anywhere = pl.BlockSpec(memory_space=pl.ANY)
    bf16, f32 = jnp.bfloat16, jnp.float32
    out = pl.pallas_call(
        functools.partial(block_kernel, head_dim),
        in_specs=[anywhere] * 6 + [pl.BlockSpec(memory_space=pltpu.VMEM)],
        out_specs=pl.BlockSpec(memory_space=pltpu.VMEM),
        out_shape=jax.ShapeDtypeStruct(chunked, f32),
        scratch_shapes=[
            pltpu.VMEM(chunked, bf16),
            pltpu.VMEM(flat, bf16),
            pltpu.VMEM(flat, bf16),
            pltpu.VMEM(flat, bf16),
            pltpu.VMEM((chunks, rows, q_width), bf16),
            pltpu.VMEM((chunks, rows, q_width), bf16),
            pltpu.VMEM((chunks, rows, v_width), bf16),
            pltpu.VMEM((chunks, rows, v_width), bf16),
            pltpu.VMEM((3 * width_win, feature_width), bf16),
            pltpu.VMEM((v_width, feature_width), bf16),
            pltpu.VMEM((3 * width_win, feature_width), bf16),
            pltpu.VMEM((width_win, feature_width), bf16),
            pltpu.VMEM((chunks, rows, v_width), f32),
            pltpu.VMEM((chunks, rows, LANES), f32),
            pltpu.VMEM((chunks, rows, LANES), f32),
            pltpu.VMEM(exchanged + (feature_width,), bf16),
            pltpu.VMEM(exchanged + (feature_width,), bf16),
            pltpu.VMEM(exchanged + (width_win,), bf16),
            pltpu.VMEM(exchanged + (width_win,), bf16),
            pltpu.SemaphoreType.DMA((6,)),
            pltpu.SemaphoreType.DMA((1,)),
            pltpu.SemaphoreType.DMA((1,)),
            pltpu.SemaphoreType.DMA((2, chunks)),
            pltpu.SemaphoreType.DMA((2, chunks)),
            pltpu.SemaphoreType.DMA((chunks, frames)),
            pltpu.SemaphoreType.DMA((chunks, frames)),
            pltpu.SemaphoreType.DMA((chunks, frames)),
            pltpu.SemaphoreType.DMA((chunks, frames)),
            pltpu.SemaphoreType.DMA((2, chunks)),
        ],
        compiler_params=pltpu.CompilerParams(
            collective_id=0, has_side_effects=True, vmem_limit_bytes=60 * 1024 * 1024
        ),
        name="denoising_block",
    )(
        tokens.reshape(chunked), stale_kv, transposed(spatial_qkv), spatial_out,
        transposed(temporal_qkv), temporal_out, mod,
    )
    return out.reshape(flat)


def solution(mesh):
    return jax.shard_map(
        per_device,
        mesh=mesh,
        in_specs=(
            P(("groups", "patch"), None),
            P(("groups", "patch"), None),
            P(),
            P(),
            P("groups"),
            P("groups"),
            P(),
            P(),
            P(),
            P(),
        ),
        out_specs=P(("groups", "patch"), None),
        check_vma=False,
    )
```
